32 devices in a mesh: grp: 4 (over y, x), dev: 8 (over z, core).
Axes of the slice: x: 2, y: 2, z: 4, core: 2. Of those that a mesh axis runs over, the one named last changes fastest.
Arguments:
- source_id: int32 [524288], P(('grp', 'dev')), may hold values from 0 to 4095, as said below
- slot: int32 [524288], P(('grp', 'dev')), may hold values from 0 to 127, as said below
- owner: int32 [4096], replicated, may hold values from 0 to 4095, as said below
- counts: int32 [4096], P(('grp', 'dev')), may hold values from 1 to 128, as said below
- partials: float32 [5, 524288], P(None, ('grp', 'dev')), may hold values from -6 to 6
- residual: float32 [524288], P(('grp', 'dev')), may hold values from -6 to 6
- weight: float32 [524288], P(('grp', 'dev')), may hold values from 0.3 to 9
- prior: float32 [5, 4096], P(None, ('grp', 'dev')), may hold values from 0.5 to 4
Outputs:
- updates: float32 [5, 4096], P(None, ('grp', 'dev'))
- standardized: float32 [524288], P(('grp', 'dev'))
- norm: float32 [], replicated
The draws below stay inside these ranges and needn't reach their ends.
Inputs may be any that keep to these rules, and one draw needn't show every extreme that they name: A permutation: source s stands at owner position owner[s], and position p belongs to device p // 128. `source_id`: the rows of one device stand in 32 aligned blocks of 512 rows; block k holds only rows whose source's owner position lies in device k's range. Over all rows, each pair of a source and a slot below 128 appears exactly once. A row is an observation when its slot is below its source's count, else padding. Each device's block of counts holds 128 at least once.
All inputs are finite; a program needn't handle non-finite values.
Results may differ from the reference program's by a relative error of at most 0.0003.
Values sent between devices are 32-bit elements; how exact they have to be, the bound alone decides.
No kernel may reach another device: no remote copies, remote signals or barrier semaphores. Data moves between devices by JAX's collectives and lax.ppermute only.
A program may use at most 64 MiB of HBM per device.

```python
import math
import jax
import jax.numpy as jnp
from jax import lax

PARAMS = 5
PAD = 128
SRC_DEV = 128
SOURCES = 4096
ROWS_DEV = 16384
ROWS_ALL = 524288
CAP = 512
N_GRP = 4
N_DEV = 8


def row_layout(key):
    base_key = jax.random.fold_in(key, 7001)
    devices_all = N_GRP * N_DEV
    placing = jax.random.permutation(jax.random.fold_in(base_key, 1), SOURCES).astype(jnp.int32)
    at_position = jnp.argsort(placing, stable=True).astype(jnp.int32)

    def owner_cells(owner_k):
        return jax.random.permutation(jax.random.fold_in(base_key, 1000 + owner_k), ROWS_DEV).astype(jnp.int32)
    cell_map = jax.vmap(owner_cells)(jnp.arange(devices_all, dtype=jnp.int32))
    cell_map = cell_map.reshape(devices_all, devices_all, CAP).transpose(1, 0, 2)
    owner_of = jnp.broadcast_to(jnp.arange(devices_all, dtype=jnp.int32)[None, :, None], cell_map.shape)
    position = owner_of * SRC_DEV + cell_map // PAD
    source_ids = at_position[position.reshape(-1)]
    slots = (cell_map % PAD).reshape(-1)
    return (placing, source_ids, slots)


def draw_owner(key, part):
    return row_layout(key)[0]


def draw_source_id(key, part):
    return row_layout(key)[1]


def draw_slot(key, part):
    return row_layout(key)[2]


def draw_counts(key, part):
    base_key = jax.random.fold_in(key, 7002)
    first_try = jax.random.randint(jax.random.fold_in(base_key, 1), (SOURCES,), 1, PAD + 1)
    second_try = jax.random.randint(jax.random.fold_in(base_key, 2), (SOURCES,), 1, PAD + 1)
    few_obs = jax.random.randint(jax.random.fold_in(base_key, 3), (SOURCES,), 1, PAD // 8 + 1)
    pick_low = jax.random.randint(jax.random.fold_in(base_key, 4), (SOURCES,), 0, 4) == 0
    result = jnp.where(pick_low, few_obs, jnp.maximum(first_try, second_try))
    full_slot = jax.random.randint(jax.random.fold_in(base_key, 5), (N_GRP * N_DEV,), 0, SRC_DEV)
    spots = jnp.arange(SOURCES, dtype=jnp.int32)
    result = jnp.where(spots % SRC_DEV == full_slot[spots // SRC_DEV], PAD, result)
    return result.astype(jnp.int32)


def draw_weight(key, part):
    row_device = jnp.arange(ROWS_ALL, dtype=jnp.int32) // ROWS_DEV
    rising = 1.0 + 2.0 * row_device.astype(jnp.float32) / max(N_GRP * N_DEV - 1, 1)
    spread = jnp.exp(jax.random.uniform(key, (ROWS_ALL,), jnp.float32, math.log(0.3), math.log(3.0)))
    return (spread * rising).astype(jnp.float32)


def steps_of(stream_key, shape, cuts, smallest, high):
    level, own = 1.0, jax.random.fold_in(stream_key, 6)
    for dim, blocks in cuts:
        heights = jnp.exp(jax.random.uniform(jax.random.fold_in(own, dim), (blocks,), jnp.float32, smallest / len(cuts), high / len(cuts)))
        level = level * jnp.repeat(heights, shape[dim] // blocks).reshape([-1 if axis == dim else 1 for axis in range(len(shape))])
    return level


def gaussian(own_key, extent, width, bound, pieces=(), kind=jnp.bfloat16):
    factor_of = steps_of(own_key, extent, pieces, -0.22, 0.18) if pieces else 1.0
    values = jax.random.normal(own_key, extent, jnp.float32) * width * factor_of
    return jnp.minimum(jnp.maximum(values, -bound), bound).astype(kind)


def setup_inputs(seed: int = 0) -> dict:
    streams_of = jax.random.split(jax.random.key(seed), 9)
    source_id = draw_source_id(jax.random.fold_in(streams_of[8], 71), 0)
    slot = draw_slot(jax.random.fold_in(streams_of[8], 71), 0)
    owner = draw_owner(jax.random.fold_in(streams_of[8], 71), 0)
    counts = draw_counts(jax.random.fold_in(streams_of[8], 71), 0)
    partials = gaussian(streams_of[4], (PARAMS, ROWS_ALL), 1.0, 6.0, ((1, 32),), jnp.float32)
    residual = gaussian(streams_of[5], (ROWS_ALL,), 1.0, 6.0, ((0, 32),), jnp.float32)
    weight = draw_weight(jax.random.fold_in(streams_of[8], 71), 0)
    prior = jnp.clip(jnp.exp(math.log(4.0) - 2.0794415 * jax.random.uniform(streams_of[7], (PARAMS, SOURCES), jnp.float32) ** steps_of(streams_of[7], (PARAMS, SOURCES), ((1, 32),), -0.2, 0.2)), 0.5, 4.0)
    return dict(source_id=source_id, slot=slot, owner=owner, counts=counts, partials=partials, residual=residual, weight=weight, prior=prior)


def solve_blocks(normal, moments):
    params = len(moments)
    factor = {}
    for column in range(params):
        running = normal[column][column]
        for earlier in range(column):
            running = running - factor[column, earlier] ** 2
        pivot_value = jnp.sqrt(running)
        factor[column, column] = pivot_value
        for target in range(column + 1, params):
            current = normal[target][column]
            for earlier in range(column):
                current = current - factor[target, earlier] * factor[column, earlier]
            factor[target, column] = current / pivot_value
    forward = []
    for target in range(params):
        current = moments[target]
        for earlier in range(target):
            current = current - factor[target, earlier] * forward[earlier]
        forward.append(current / factor[target, target])
    backward = [None] * params
    for target in reversed(range(params)):
        current = forward[target]
        for later in range(target + 1, params):
            current = current - factor[later, target] * backward[later]
        backward[target] = current / factor[target, target]
    return jnp.stack(backward)

def reference(source_id, slot, owner, counts, partials, residual, weight, prior):
    params = partials.shape[0]
    position = owner[source_id]
    live_mask = (slot < counts[position]).astype(jnp.float32)
    weighted = partials * (weight * live_mask)[None, :]
    normal = [[None] * params for _ in range(params)]
    for first_idx in range(params):
        for second_idx in range(first_idx, params):
            entry = jax.ops.segment_sum(weighted[first_idx] * partials[second_idx], position, num_segments=SOURCES)
            if first_idx == second_idx:
                entry = entry + prior[first_idx]
            normal[first_idx][second_idx] = entry
            normal[second_idx][first_idx] = entry
    moments = [jax.ops.segment_sum(weighted[first_idx] * residual, position, num_segments=SOURCES) for first_idx in range(params)]
    updates = solve_blocks(normal, moments)
    fitted = lax.optimization_barrier(jnp.sum(partials * updates[:, position], axis=0))
    fresh = (residual - fitted) * live_mask
    squares = jnp.sum(weight * fresh * fresh)
    live_total = jnp.sum(live_mask)
    norm = jnp.sqrt(squares / live_total + 1e-06)
    return (updates, fresh * jnp.sqrt(weight) / norm, norm)
```

```python
import jax
import jax.numpy as jnp
from jax import lax
from jax.experimental import pallas as pl
from jax.experimental.pallas import tpu as pltpu
from jax.sharding import PartitionSpec as P

LANES = 128
SUB = 8


def pick_lanes(table, idx):
    return jnp.take_along_axis(table, idx, axis=1, mode="promise_in_bounds")


def pack_kernel(sid_ref, slot_ref, owner_ref, partials_ref, res_ref, wgt_ref, wire_ref, *, src_local, pad_slots):
    params = partials_ref.shape[0]
    table_tiles = owner_ref.shape[0] // SUB
    row_of = lax.broadcasted_iota(jnp.int32, (SUB, LANES), 0)

    def group(g, carry):
        base = pl.multiple_of(g * SUB, SUB)
        sid = sid_ref[pl.ds(base, SUB), :]
        low = sid % LANES
        high = sid // LANES

        def look(t, pos):
            tile = owner_ref[pl.ds(pl.multiple_of(t * SUB, SUB), SUB), :]
            for s in range(SUB):
                line = jnp.broadcast_to(tile[s : s + 1, :], (SUB, LANES))
                pos = jnp.where(high == t * SUB + s, pick_lanes(line, low), pos)
            return pos

        pos = jnp.zeros((SUB, LANES), jnp.int32)
        if table_tiles <= 4:
            for t in range(table_tiles):
                pos = look(t, pos)
        else:
            pos = lax.fori_loop(0, table_tiles, look, pos)
        cell = (pos % src_local * pad_slots + slot_ref[pl.ds(base, SUB), :]).astype(jnp.float32)
        res = res_ref[pl.ds(base, SUB), :]
        wgt = wgt_ref[pl.ds(base, SUB), :]
        for s in range(SUB):
            lane0 = pl.multiple_of((base + s) * LANES, LANES)
            slopes = partials_ref[:, pl.ds(lane0, LANES)]
            tile = jnp.concatenate([slopes, jnp.zeros((SUB - params, LANES), jnp.float32)], axis=0)
            tile = jnp.where(row_of == params, res[s : s + 1, :], tile)
            tile = jnp.where(row_of == params + 1, wgt[s : s + 1, :], tile)
            tile = jnp.where(row_of == params + 2, cell[s : s + 1, :], tile)
            wire_ref[base + s] = tile
        return carry

    lax.fori_loop(0, sid_ref.shape[0] // SUB, group, 0)


def solve_rows(normal, moments):
    params = len(moments)
    factor = {}
    for column in range(params):
        running = normal[column][column]
        for earlier in range(column):
            running = running - factor[column, earlier] ** 2
        pivot_value = jnp.sqrt(running)
        factor[column, column] = pivot_value
        for target in range(column + 1, params):
            current = normal[target][column]
            for earlier in range(column):
                current = current - factor[target, earlier] * factor[column, earlier]
            factor[target, column] = current / pivot_value
    forward = []
    for target in range(params):
        current = moments[target]
        for earlier in range(target):
            current = current - factor[target, earlier] * forward[earlier]
        forward.append(current / factor[target, target])
    backward = [None] * params
    for target in reversed(range(params)):
        current = forward[target]
        for later in range(target + 1, params):
            current = current - factor[later, target] * backward[later]
        backward[target] = current / factor[target, target]
    return backward


def owner_kernel(wire_ref, counts_ref, prior_ref, upd_ref, out_ref, acc_ref, live_ref, *, pad_slots, per):
    params = prior_ref.shape[0]
    chunks = wire_ref.shape[0]
    src_local = counts_ref.shape[1]
    row_of = lax.broadcasted_iota(jnp.int32, (SUB, LANES), 0)
    source_of = lax.broadcasted_iota(jnp.int32, (src_local, LANES), 0)
    counts = counts_ref[...]
    count_table = jnp.broadcast_to(counts, (SUB, src_local))
    acc_ref[...] = jnp.zeros_like(acc_ref)

    def cell_of(tile):
        cell = jnp.broadcast_to(tile[params + 2 : params + 3, :].astype(jnp.int32), (SUB, LANES))
        return cell // pad_slots, cell % pad_slots

    step = 8

    def gather_sums(index, carry):
        lefts, hots = [], []
        for s in range(step):
            chunk = index * step + s
            tile = wire_ref[chunk]
            source, slot = cell_of(tile)
            live = (slot < pick_lanes(count_table, source)).astype(jnp.float32)
            live_ref[chunk] = live
            scaled = tile * (tile[params + 1 : params + 2, :] * live)
            turn1 = jnp.concatenate([tile[1:params], tile[0:1], tile[params:]], axis=0)
            turn2 = jnp.concatenate([tile[2:params], tile[0:2], tile[params:]], axis=0)
            stats = jnp.concatenate(
                [scaled * tile, scaled * turn1, scaled * turn2, scaled * tile[params : params + 1, :]],
                axis=0,
            )
            first = stats.astype(jnp.bfloat16)
            rest = stats - first.astype(jnp.float32)
            second = rest.astype(jnp.bfloat16)
            third = (rest - second.astype(jnp.float32)).astype(jnp.bfloat16)
            lefts.append(jnp.concatenate([first, second, third], axis=0))
            hots.append((source_of == source[0:1, :]).astype(jnp.float32).astype(jnp.bfloat16))
        acc_ref[...] += lax.dot_general(
            jnp.concatenate(lefts, axis=1),
            jnp.concatenate(hots, axis=1),
            (((1,), (1,)), ((), ())),
            preferred_element_type=jnp.float32,
        )
        return carry

    lax.fori_loop(0, chunks // step, gather_sums, 0)
    width = 4 * SUB
    sums = acc_ref[0:width, :] + (acc_ref[width : 2 * width, :] + acc_ref[2 * width : 3 * width, :])
    normal = [[None] * params for _ in range(params)]
    for turn in range(3):
        for first_idx in range(params):
            second_idx = (first_idx + turn) % params
            entry = sums[turn * SUB + first_idx : turn * SUB + first_idx + 1, :]
            if turn == 0:
                entry = entry + prior_ref[first_idx : first_idx + 1, :]
            normal[first_idx][second_idx] = entry
            normal[second_idx][first_idx] = entry
    moments = [sums[3 * SUB + i : 3 * SUB + i + 1, :] for i in range(params)]
    solved = solve_rows(normal, moments)
    table = jnp.zeros((SUB, src_local), jnp.float32)
    for i in range(params):
        upd_ref[i : i + 1, :] = solved[i]
        table = jnp.where(row_of == i, solved[i], table)

    def refit(index, total):
        for s in range(step):
            chunk = index * step + s
            tile = wire_ref[chunk]
            source, _ = cell_of(tile)
            fitted = jnp.sum(
                jnp.where(row_of < params, tile * pick_lanes(table, source), 0.0), axis=0, keepdims=True
            )
            fresh = (tile[params : params + 1, :] - fitted) * live_ref[chunk][0:1, :]
            total = total + tile[params + 1 : params + 2, :] * fresh * fresh
            if per:
                out_ref[chunk // per, pl.ds(chunk % per, 1), :] = fresh
            else:
                out_ref[pl.ds(chunk, 1), :] = fresh
        return total

    total = lax.fori_loop(0, chunks // step, refit, jnp.zeros((1, LANES), jnp.float32))
    squares = jnp.sum(total, axis=1, keepdims=True)
    seen = jnp.sum(counts.astype(jnp.float32), axis=1, keepdims=True)
    lane_of = lax.broadcasted_iota(jnp.int32, (1, LANES), 1)
    line = jnp.where(lane_of == 0, squares, jnp.where(lane_of == 1, seen, 0.0))
    if per:
        for peer in range(out_ref.shape[0]):
            out_ref[peer, per : per + 1, :] = line
    else:
        out_ref[chunks : chunks + 1, :] = line


def finish_kernel(back_ref, wgt_ref, std_ref, norm_ref, *, per):
    peers = back_ref.shape[0]
    lines = jnp.sum(back_ref[:, per, :], axis=0, keepdims=True)
    lane_of = lax.broadcasted_iota(jnp.int32, (1, LANES), 1)
    squares = jnp.sum(jnp.where(lane_of == 0, lines, 0.0), axis=1, keepdims=True)
    seen = jnp.sum(jnp.where(lane_of == 1, lines, 0.0), axis=1, keepdims=True)
    norm = jnp.sqrt(squares / seen + 1e-06)
    norm_ref[...] = norm
    for peer in range(peers):
        rows = slice(peer * per, (peer + 1) * per)
        std_ref[rows, :] = back_ref[peer, 0:per, :] * jnp.sqrt(wgt_ref[rows, :]) / norm


def body(source_id, slot, owner, counts, partials, residual, weight, prior):
    axes = ("grp", "dev")
    peers = lax.axis_size("grp") * lax.axis_size("dev")
    params = partials.shape[0]
    row_count = residual.shape[0]
    src_local = counts.shape[0]
    pad_slots = row_count // src_local
    block_rows = row_count // peers
    chunks = row_count // LANES
    per = block_rows // LANES
    f32 = jnp.float32
    grid_of = lambda x: x.reshape(-1, LANES)
    wgt = grid_of(weight)
    wire = pl.pallas_call(
        lambda *refs: pack_kernel(*refs, src_local=src_local, pad_slots=pad_slots),
        out_shape=jax.ShapeDtypeStruct((chunks, SUB, LANES), f32),
        name="pack_rows",
    )(grid_of(source_id), grid_of(slot), grid_of(owner), partials, grid_of(residual), wgt)
    if per:
        arrived = lax.all_to_all(
            wire.reshape(peers, per, SUB, LANES), axes, split_axis=0, concat_axis=0, tiled=True
        ).reshape(chunks, SUB, LANES)
    else:
        parts = LANES // block_rows
        cut = wire.reshape(chunks, SUB, parts, block_rows).transpose(0, 2, 1, 3)
        cut = lax.all_to_all(
            cut.reshape(peers, SUB, block_rows), axes, split_axis=0, concat_axis=0, tiled=True
        )
        cut = cut.reshape(chunks, parts, SUB, block_rows).transpose(0, 2, 1, 3)
        arrived = cut.reshape(chunks, SUB, LANES)
    back_shape = (peers, per + 1, LANES) if per else (chunks + 1, LANES)
    updates, back = pl.pallas_call(
        lambda *refs: owner_kernel(*refs, pad_slots=pad_slots, per=per),
        out_shape=(
            jax.ShapeDtypeStruct((params, src_local), f32),
            jax.ShapeDtypeStruct(back_shape, f32),
        ),
        scratch_shapes=[
            pltpu.VMEM((12 * SUB, src_local), f32),
            pltpu.VMEM((chunks, SUB, LANES), f32),
        ],
        name="owner_fit",
    )(arrived, counts.reshape(1, -1), prior)
    if per:
        back = lax.all_to_all(back, axes, split_axis=0, concat_axis=0, tiled=True)
        standardized, norm = pl.pallas_call(
            lambda *refs: finish_kernel(*refs, per=per),
            out_shape=(
                jax.ShapeDtypeStruct((chunks, LANES), f32),
                jax.ShapeDtypeStruct((1, 1), f32),
            ),
            name="finish",
        )(back, wgt)
        return (updates, standardized.reshape(row_count), norm.reshape(()))
    line = jnp.broadcast_to(back[chunks, 0:2][None], (peers, 2))
    back = jnp.concatenate([back[:chunks].reshape(peers, block_rows), line], axis=1)
    back = lax.all_to_all(back, axes, split_axis=0, concat_axis=0, tiled=True)
    totals = jnp.sum(back[:, block_rows:], axis=0)
    norm = jnp.sqrt(totals[0] / totals[1] + 1e-06)
    fresh = back[:, :block_rows].reshape(row_count)
    return (updates, fresh * jnp.sqrt(weight) / norm, norm)


def solution(mesh):
    in_specs = (
        P(("grp", "dev")),
        P(("grp", "dev")),
        P(),
        P(("grp", "dev")),
        P(None, ("grp", "dev")),
        P(("grp", "dev")),
        P(("grp", "dev")),
        P(None, ("grp", "dev")),
    )
    out_specs = (P(None, ("grp", "dev")), P(("grp", "dev")), P())
    return jax.shard_map(body, mesh=mesh, in_specs=in_specs, out_specs=out_specs, check_vma=False)
```

```python
import jax
import jax.numpy as jnp
from jax import lax
from jax.experimental import pallas as pl
from jax.experimental.pallas import tpu as pltpu
from jax.sharding import PartitionSpec as P

LANES = 128
SUB = 8
QUAD = 4


def pick_lanes(table, idx):
    return jnp.take_along_axis(table, idx, axis=1, mode="promise_in_bounds")


def split_index(value, size):
    if size & (size - 1) == 0:
        return lax.shift_right_logical(value, size.bit_length() - 1), value & (size - 1)
    return lax.div(value, size), lax.rem(value, size)


def pack_kernel(sid_ref, slot_ref, owner_ref, partials_ref, res_ref, wgt_ref, wire_ref, *, src_local, pad_slots, compact):
    params = partials_ref.shape[0]
    bits = max(1, (src_local - 1).bit_length())
    fit = 31 // bits
    tiles = owner_ref.shape[0] // SUB
    row_of = lax.broadcasted_iota(jnp.int32, (SUB, LANES), 0)

    def merged(first, count):
        line = jnp.zeros((SUB, LANES), jnp.int32)
        for t in range(count):
            here = owner_ref[pl.ds(pl.multiple_of((first + t) * SUB, SUB), SUB), :]
            line = line | (split_index(here, src_local)[1] << (t * bits))
        return line

    def look(first, count, high, low, pos):
        packed = merged(first, count)
        tile_id, line_id = split_index(high, SUB)
        found = jnp.zeros((SUB, LANES), jnp.int32)
        for s in range(SUB):
            line = jnp.broadcast_to(packed[s : s + 1, :], (SUB, LANES))
            found = jnp.where(line_id == s, pick_lanes(line, low), found)
        turn = tile_id - first
        inside = (turn >= 0) & (turn < count)
        moved = lax.shift_right_logical(found, jnp.where(inside, turn, 0) * bits) & ((1 << bits) - 1)
        return jnp.where(inside, moved, pos)

    def group(g, carry):
        base = pl.multiple_of(g * SUB, SUB)
        high, low = split_index(sid_ref[pl.ds(base, SUB), :], LANES)
        pos = jnp.zeros((SUB, LANES), jnp.int32)
        whole = tiles // fit
        if whole <= 1:
            for t in range(whole):
                pos = look(t * fit, fit, high, low, pos)
        else:
            pos = lax.fori_loop(0, whole, lambda t, p: look(t * fit, fit, high, low, p), pos)
        if tiles % fit:
            pos = look(whole * fit, tiles % fit, high, low, pos)
        cell = (pos * pad_slots + slot_ref[pl.ds(base, SUB), :]).astype(jnp.float32)
        root = jnp.sqrt(wgt_ref[pl.ds(base, SUB), :])
        res = res_ref[pl.ds(base, SUB), :] * root
        built = []
        for s in range(SUB):
            lane0 = pl.multiple_of((base + s) * LANES, LANES)
            slopes = partials_ref[:, pl.ds(lane0, LANES)] * root[s : s + 1, :]
            tile = jnp.concatenate([slopes, jnp.zeros((SUB - params, LANES), jnp.float32)], axis=0)
            tile = jnp.where(row_of == params, res[s : s + 1, :], tile)
            built.append(jnp.where(row_of == params + 1, cell[s : s + 1, :], tile))
        if not compact:
            for s in range(SUB):
                wire_ref[base + s] = built[s]
            return carry
        for quad in range(SUB // QUAD):
            last = built[quad * QUAD + QUAD - 1]
            line0 = (g * (SUB // QUAD) + quad) * (2 * QUAD - 1)
            for c in range(QUAD - 1):
                tile = jnp.where(row_of == SUB - 1, last[QUAD + c : QUAD + c + 1, :], built[quad * QUAD + c])
                wire_ref[line0 + 2 * c] = tile[0:QUAD]
                wire_ref[line0 + 2 * c + 1] = tile[QUAD:]
            wire_ref[line0 + 2 * QUAD - 2] = last[0:QUAD]
        return carry

    lax.fori_loop(0, sid_ref.shape[0] // SUB, group, 0)


def solve_rows(normal, moments):
    params = len(moments)
    raw, factor, inverse = {}, {}, []
    for column in range(params):
        for target in range(column, params):
            current = normal[target][column]
            for earlier in range(column):
                current = current - factor[target, earlier] * raw[column, earlier]
            raw[target, column] = current
        inverse.append(1.0 / raw[column, column])
        for target in range(column + 1, params):
            factor[target, column] = raw[target, column] * inverse[column]
    forward = []
    for target in range(params):
        current = moments[target]
        for earlier in range(target):
            current = current - factor[target, earlier] * forward[earlier]
        forward.append(current)
    backward = [None] * params
    for target in reversed(range(params)):
        current = forward[target] * inverse[target]
        for later in range(target + 1, params):
            current = current - factor[later, target] * backward[later]
        backward[target] = current
    return backward


def owner_kernel(wire_ref, counts_ref, prior_ref, upd_ref, out_ref, acc_ref, rows_ref, src_ref, *, pad_slots, per, compact):
    params = prior_ref.shape[0]
    chunks = rows_ref.shape[0]
    src_local = counts_ref.shape[1]
    row_of = lax.broadcasted_iota(jnp.int32, (SUB, LANES), 0)
    source_of = lax.broadcasted_iota(jnp.int32, (src_local, LANES), 0)
    counts = counts_ref[...]
    count_table = jnp.broadcast_to(counts, (SUB, src_local))
    acc_ref[...] = jnp.zeros_like(acc_ref)
    step = SUB

    def tiles_of(index):
        if not compact:
            return [wire_ref[index * step + s] for s in range(step)]
        out = []
        for quad in range(step // QUAD):
            line0 = (index * (step // QUAD) + quad) * (2 * QUAD - 1)
            three = [
                jnp.concatenate([wire_ref[line0 + 2 * c], wire_ref[line0 + 2 * c + 1]], axis=0)
                for c in range(QUAD - 1)
            ]
            spare = [tile[SUB - 1 :, :] for tile in three]
            last = jnp.concatenate([wire_ref[line0 + 2 * QUAD - 2]] + spare + [spare[0]], axis=0)
            out += three + [last]
        return out

    def gather_sums(index, carry):
        lefts, hots = [], []
        for s, tile in enumerate(tiles_of(index)):
            chunk = index * step + s
            cell = jnp.broadcast_to(tile[params + 1 : params + 2, :].astype(jnp.int32), (SUB, LANES))
            source, slot = split_index(cell, pad_slots)
            rows = jnp.where(slot < pick_lanes(count_table, source), tile, 0.0)
            rows_ref[chunk] = rows
            src_ref[chunk] = source
            left = jnp.where(row_of < params, rows, rows[params : params + 1, :])
            turn = lambda shift: pltpu.roll(rows, shift, 0)
            right0 = jnp.where(row_of < params, rows, turn(5))
            right1 = jnp.where(row_of < 4, turn(7), jnp.where(row_of == 4, turn(4), turn(2)))
            right2 = jnp.where(row_of < 3, turn(6), turn(3))
            parts = [left * right0, left * right1, left * right2]
            pieces = []
            for _ in range(2):
                heads = [p.astype(jnp.bfloat16).astype(jnp.float32) for p in parts]
                pieces += heads
                parts = [p - h for p, h in zip(parts, heads)]
            lefts.append(jnp.concatenate(pieces + parts, axis=0).astype(jnp.bfloat16))
            hots.append((source_of == source[0:1, :]).astype(jnp.float32).astype(jnp.bfloat16))
        acc_ref[...] += lax.dot_general(
            jnp.concatenate(lefts, axis=1),
            jnp.concatenate(hots, axis=1),
            (((1,), (1,)), ((), ())),
            preferred_element_type=jnp.float32,
        )
        return carry

    lax.fori_loop(0, chunks // step, gather_sums, 0)
    width = 3 * SUB
    sums = acc_ref[0:width, :] + (acc_ref[width : 2 * width, :] + acc_ref[2 * width : 3 * width, :])
    line_at = lambda turn, row: sums[turn * SUB + row : turn * SUB + row + 1, :]
    normal = [[None] * params for _ in range(params)]
    for turn in range(3):
        for first_idx in range(params):
            second_idx = (first_idx + turn) % params
            entry = line_at(turn, first_idx)
            if turn == 0:
                entry = entry + prior_ref[first_idx : first_idx + 1, :]
            normal[first_idx][second_idx] = entry
            normal[second_idx][first_idx] = entry
    moments = [line_at(0, 5), line_at(0, 6), line_at(0, 7), line_at(1, 5), line_at(1, 6)]
    solved = solve_rows(normal, moments)
    table = jnp.where(row_of == params, 1.0, 0.0)
    for i in range(params):
        upd_ref[i : i + 1, :] = solved[i]
        table = jnp.where(row_of == i, -solved[i], table)

    def refit(index, total):
        for s in range(step):
            chunk = index * step + s
            fresh = jnp.sum(rows_ref[chunk] * pick_lanes(table, src_ref[chunk]), axis=0, keepdims=True)
            total = total + fresh * fresh
            out_ref[chunk + (chunk // per if per else 0)] = fresh
        return total

    total = lax.fori_loop(0, chunks // step, refit, jnp.zeros((1, LANES), jnp.float32))
    squares = jnp.sum(total, axis=1, keepdims=True)
    seen = jnp.sum(counts.astype(jnp.float32), axis=1, keepdims=True)
    lane_of = lax.broadcasted_iota(jnp.int32, (1, LANES), 1)
    line = jnp.where(lane_of == 0, squares, jnp.where(lane_of == 1, seen, 0.0))
    stride = per + 1 if per else chunks + 1
    for last in range(stride - 1, out_ref.shape[0], stride):
        out_ref[last] = line


def finish_kernel(back_ref, std_ref, norm_ref, *, per):
    stride = per + 1
    lines = [back_ref[last] for last in range(per, back_ref.shape[0], stride)]
    while len(lines) > 1:
        lines = [a + b for a, b in zip(lines[::2], lines[1::2])] + lines[len(lines) & ~1 :]
    lane_of = lax.broadcasted_iota(jnp.int32, (1, LANES), 1)
    squares = jnp.sum(jnp.where(lane_of == 0, lines[0], 0.0), axis=1, keepdims=True)
    seen = jnp.sum(jnp.where(lane_of == 1, lines[0], 0.0), axis=1, keepdims=True)
    norm = jnp.sqrt(squares / seen + 1e-06)
    norm_ref[...] = norm
    inverse = jnp.broadcast_to(1.0 / norm, (1, LANES))
    for chunk in range(std_ref.shape[0]):
        std_ref[chunk : chunk + 1, :] = back_ref[chunk + chunk // per] * inverse


def body(source_id, slot, owner, counts, partials, residual, weight, prior):
    axes = ("grp", "dev")
    peers = lax.axis_size("grp") * lax.axis_size("dev")
    params = partials.shape[0]
    row_count = residual.shape[0]
    src_local = counts.shape[0]
    pad_slots = row_count // src_local
    block_rows = row_count // peers
    chunks = row_count // LANES
    per = block_rows // LANES
    compact = per > 0 and per % QUAD == 0
    f32 = jnp.float32
    grid_of = lambda x: x.reshape(-1, LANES)
    send = lambda x: lax.all_to_all(x, axes, split_axis=0, concat_axis=0, tiled=True)
    vmem_spec = pl.BlockSpec(memory_space=pltpu.VMEM)
    wire_shape = (chunks // QUAD * (2 * QUAD - 1), QUAD, LANES) if compact else (chunks, SUB, LANES)
    wire = pl.pallas_call(
        lambda *refs: pack_kernel(*refs, src_local=src_local, pad_slots=pad_slots, compact=compact),
        out_shape=pltpu.VMEM(wire_shape, f32),
        name="pack_rows",
    )(grid_of(source_id), grid_of(slot), grid_of(owner), partials, grid_of(residual), grid_of(weight))
    if per:
        arrived = send(wire.reshape((peers, -1) + wire_shape[1:])).reshape(wire_shape)
    else:
        parts = LANES // block_rows
        cut = wire.reshape(chunks, SUB, parts, block_rows).transpose(0, 2, 1, 3)
        cut = send(cut.reshape(peers, SUB, block_rows))
        cut = cut.reshape(chunks, parts, SUB, block_rows).transpose(0, 2, 1, 3)
        arrived = cut.reshape(wire_shape)
    back_lines = peers * (per + 1) if per else chunks + 1
    updates, back = pl.pallas_call(
        lambda *refs: owner_kernel(*refs, pad_slots=pad_slots, per=per, compact=compact),
        out_shape=(
            jax.ShapeDtypeStruct((params, src_local), f32),
            pltpu.VMEM((back_lines, 1, LANES), f32),
        ),
        in_specs=[vmem_spec] * 3,
        scratch_shapes=[
            pltpu.VMEM((9 * SUB, src_local), f32),
            pltpu.VMEM((chunks, SUB, LANES), f32),
            pltpu.VMEM((chunks, SUB, LANES), jnp.int32),
        ],
        name="owner_fit",
    )(arrived, counts.reshape(1, -1), prior)
    if per:
        back = send(back.reshape(peers, per + 1, 1, LANES)).reshape(back_lines, 1, LANES)
        standardized, norm = pl.pallas_call(
            lambda *refs: finish_kernel(*refs, per=per),
            out_shape=(
                jax.ShapeDtypeStruct((chunks, LANES), f32),
                jax.ShapeDtypeStruct((1, 1), f32),
            ),
            in_specs=[vmem_spec],
            name="finish",
        )(back)
        return (updates, standardized.reshape(row_count), norm.reshape(()))
    back = back[:, 0, :]
    line = jnp.broadcast_to(back[chunks, 0:2][None], (peers, 2))
    back = send(jnp.concatenate([back[:chunks].reshape(peers, block_rows), line], axis=1))
    totals = jnp.sum(back[:, block_rows:], axis=0)
    norm = jnp.sqrt(totals[0] / totals[1] + 1e-06)
    return (updates, back[:, :block_rows].reshape(row_count) / norm, norm)


def solution(mesh):
    in_specs = (
        P(("grp", "dev")),
        P(("grp", "dev")),
        P(),
        P(("grp", "dev")),
        P(None, ("grp", "dev")),
        P(("grp", "dev")),
        P(("grp", "dev")),
        P(None, ("grp", "dev")),
    )
    out_specs = (P(None, ("grp", "dev")), P(("grp", "dev")), P())
    return jax.shard_map(body, mesh=mesh, in_specs=in_specs, out_specs=out_specs, check_vma=False)
```

```python
import jax
import jax.numpy as jnp
from jax import lax
from jax.experimental import pallas as pl
from jax.experimental.pallas import tpu as pltpu
from jax.sharding import PartitionSpec as P

LANES = 128
SUB = 8
QUAD = 4
STEP = 128


def pick_lanes(table, idx):
    return jnp.take_along_axis(table, idx, axis=1, mode="promise_in_bounds")


def split_index(value, size):
    if size & (size - 1) == 0:
        return lax.shift_right_logical(value, size.bit_length() - 1), value & (size - 1)
    return lax.div(value, size), lax.rem(value, size)


def pack_kernel(sid_ref, slot_ref, owner_ref, partials_ref, res_ref, wgt_ref, wire_ref, *, src_local, pad_slots, compact):
    params = partials_ref.shape[0]
    bits = max(1, (src_local - 1).bit_length())
    fit = 31 // bits
    tiles = owner_ref.shape[0] // SUB
    row_of = lax.broadcasted_iota(jnp.int32, (SUB, LANES), 0)

    def merged(first, count):
        line = jnp.zeros((SUB, LANES), jnp.int32)
        for t in range(count):
            here = owner_ref[pl.ds(pl.multiple_of((first + t) * SUB, SUB), SUB), :]
            line = line | (split_index(here, src_local)[1] << (t * bits))
        return line

    def look(first, count, high, low, pos):
        packed = merged(first, count)
        tile_id, line_id = split_index(high, SUB)
        found = jnp.zeros((SUB, LANES), jnp.int32)
        for s in range(SUB):
            line = jnp.broadcast_to(packed[s : s + 1, :], (SUB, LANES))
            found = jnp.where(line_id == s, pick_lanes(line, low), found)
        turn = tile_id - first
        inside = (turn >= 0) & (turn < count)
        moved = lax.shift_right_logical(found, jnp.where(inside, turn, 0) * bits) & ((1 << bits) - 1)
        return jnp.where(inside, moved, pos)

    def group(g, carry):
        base = pl.multiple_of(g * SUB, SUB)
        high, low = split_index(sid_ref[pl.ds(base, SUB), :], LANES)
        pos = jnp.zeros((SUB, LANES), jnp.int32)
        whole = tiles // fit
        if whole <= 1:
            for t in range(whole):
                pos = look(t * fit, fit, high, low, pos)
        else:
            pos = lax.fori_loop(0, whole, lambda t, p: look(t * fit, fit, high, low, p), pos)
        if tiles % fit:
            pos = look(whole * fit, tiles % fit, high, low, pos)
        cell = (pos * pad_slots + slot_ref[pl.ds(base, SUB), :]).astype(jnp.float32)
        root = jnp.sqrt(wgt_ref[pl.ds(base, SUB), :])
        res = res_ref[pl.ds(base, SUB), :] * root
        built = []
        for s in range(SUB):
            lane0 = pl.multiple_of((base + s) * LANES, LANES)
            slopes = partials_ref[:, pl.ds(lane0, LANES)] * root[s : s + 1, :]
            tile = jnp.concatenate([slopes, jnp.zeros((SUB - params, LANES), jnp.float32)], axis=0)
            tile = jnp.where(row_of == params, res[s : s + 1, :], tile)
            built.append(jnp.where(row_of == params + 1, cell[s : s + 1, :], tile))
        if not compact:
            for s in range(SUB):
                wire_ref[base + s] = built[s]
            return carry
        for quad in range(SUB // QUAD):
            last = built[quad * QUAD + QUAD - 1]
            line0 = (g * (SUB // QUAD) + quad) * (2 * QUAD - 1)
            for c in range(QUAD - 1):
                tile = jnp.where(row_of == SUB - 1, last[QUAD + c : QUAD + c + 1, :], built[quad * QUAD + c])
                wire_ref[line0 + 2 * c] = tile[0:QUAD]
                wire_ref[line0 + 2 * c + 1] = tile[QUAD:]
            wire_ref[line0 + 2 * QUAD - 2] = last[0:QUAD]
        return carry

    lax.fori_loop(0, sid_ref.shape[0] // SUB, group, 0, unroll=16)


def solve_rows(normal, moments):
    params = len(moments)
    raw, factor, inverse = {}, {}, []
    for column in range(params):
        for target in range(column, params):
            current = normal[target][column]
            for earlier in range(column):
                current = current - factor[target, earlier] * raw[column, earlier]
            raw[target, column] = current
        inverse.append(1.0 / raw[column, column])
        for target in range(column + 1, params):
            factor[target, column] = raw[target, column] * inverse[column]
    forward = []
    for target in range(params):
        current = moments[target]
        for earlier in range(target):
            current = current - factor[target, earlier] * forward[earlier]
        forward.append(current)
    backward = [None] * params
    for target in reversed(range(params)):
        current = forward[target] * inverse[target]
        for later in range(target + 1, params):
            current = current - factor[later, target] * backward[later]
        backward[target] = current
    return backward


def owner_kernel(wire_ref, counts_ref, prior_ref, upd_ref, out_ref, acc_ref, rows_ref, src_ref, *, pad_slots, per, compact):
    params = prior_ref.shape[0]
    chunks = rows_ref.shape[0]
    src_local = counts_ref.shape[1]
    row_of = lax.broadcasted_iota(jnp.int32, (SUB, LANES), 0)
    source_of = lax.broadcasted_iota(jnp.int32, (src_local, LANES), 0)
    counts = counts_ref[...]
    count_table = jnp.broadcast_to(counts, (SUB, src_local))
    acc_ref[...] = jnp.zeros_like(acc_ref)
    step = min(STEP, chunks)

    def tiles_of(index):
        if not compact:
            return [wire_ref[index * step + s] for s in range(step)]
        out = []
        for quad in range(step // QUAD):
            line0 = (index * (step // QUAD) + quad) * (2 * QUAD - 1)
            three = [
                jnp.concatenate([wire_ref[line0 + 2 * c], wire_ref[line0 + 2 * c + 1]], axis=0)
                for c in range(QUAD - 1)
            ]
            spare = [tile[SUB - 1 :, :] for tile in three]
            last = jnp.concatenate([wire_ref[line0 + 2 * QUAD - 2]] + spare + [spare[0]], axis=0)
            out += three + [last]
        return out

    def gather_sums(index, carry):
        lefts, hots = [], []
        for s, tile in enumerate(tiles_of(index)):
            chunk = index * step + s
            cell = jnp.broadcast_to(tile[params + 1 : params + 2, :].astype(jnp.int32), (SUB, LANES))
            source, slot = split_index(cell, pad_slots)
            rows = jnp.where(slot < pick_lanes(count_table, source), tile, 0.0)
            rows_ref[chunk] = rows
            src_ref[chunk] = source
            left = jnp.where(row_of < params, rows, rows[params : params + 1, :])
            turn = lambda shift: pltpu.roll(rows, shift, 0)
            right0 = jnp.where(row_of < params, rows, turn(5))
            right1 = jnp.where(row_of < 4, turn(7), jnp.where(row_of == 4, turn(4), turn(2)))
            right2 = jnp.where(row_of < 3, turn(6), turn(3))
            parts = [left * right0, left * right1, left * right2]
            pieces = []
            for _ in range(2):
                heads = [p.astype(jnp.bfloat16).astype(jnp.float32) for p in parts]
                pieces += heads
                parts = [p - h for p, h in zip(parts, heads)]
            lefts.append(jnp.concatenate(pieces + parts, axis=0).astype(jnp.bfloat16))
            hots.append((source_of == source[0:1, :]).astype(jnp.float32).astype(jnp.bfloat16))
        acc_ref[...] += lax.dot_general(
            jnp.concatenate(lefts, axis=1),
            jnp.concatenate(hots, axis=1),
            (((1,), (1,)), ((), ())),
            preferred_element_type=jnp.float32,
        )
        return carry

    lax.fori_loop(0, chunks // step, gather_sums, 0)
    width = 3 * SUB
    sums = acc_ref[0:width, :] + (acc_ref[width : 2 * width, :] + acc_ref[2 * width : 3 * width, :])
    line_at = lambda turn, row: sums[turn * SUB + row : turn * SUB + row + 1, :]
    normal = [[None] * params for _ in range(params)]
    for turn in range(3):
        for first_idx in range(params):
            second_idx = (first_idx + turn) % params
            entry = line_at(turn, first_idx)
            if turn == 0:
                entry = entry + prior_ref[first_idx : first_idx + 1, :]
            normal[first_idx][second_idx] = entry
            normal[second_idx][first_idx] = entry
    moments = [line_at(0, 5), line_at(0, 6), line_at(0, 7), line_at(1, 5), line_at(1, 6)]
    solved = solve_rows(normal, moments)
    table = jnp.where(row_of == params, 1.0, 0.0)
    for i in range(params):
        upd_ref[i : i + 1, :] = solved[i]
        table = jnp.where(row_of == i, -solved[i], table)

    def refit(index, total):
        for s in range(step):
            chunk = index * step + s
            fresh = jnp.sum(rows_ref[chunk] * pick_lanes(table, src_ref[chunk]), axis=0, keepdims=True)
            total = total + fresh * fresh
            out_ref[chunk + (chunk // per if per else 0)] = fresh
        return total

    total = lax.fori_loop(0, chunks // step, refit, jnp.zeros((1, LANES), jnp.float32))
    squares = jnp.sum(total, axis=1, keepdims=True)
    seen = jnp.sum(counts.astype(jnp.float32), axis=1, keepdims=True)
    lane_of = lax.broadcasted_iota(jnp.int32, (1, LANES), 1)
    line = jnp.where(lane_of == 0, squares, jnp.where(lane_of == 1, seen, 0.0))
    stride = per + 1 if per else chunks + 1
    for last in range(stride - 1, out_ref.shape[0], stride):
        out_ref[last] = line


def finish_kernel(back_ref, std_ref, norm_ref, *, per):
    stride = per + 1
    lines = [back_ref[last] for last in range(per, back_ref.shape[0], stride)]
    while len(lines) > 1:
        lines = [a + b for a, b in zip(lines[::2], lines[1::2])] + lines[len(lines) & ~1 :]
    lane_of = lax.broadcasted_iota(jnp.int32, (1, LANES), 1)
    squares = jnp.sum(jnp.where(lane_of == 0, lines[0], 0.0), axis=1, keepdims=True)
    seen = jnp.sum(jnp.where(lane_of == 1, lines[0], 0.0), axis=1, keepdims=True)
    norm = jnp.sqrt(squares / seen + 1e-06)
    norm_ref[...] = norm
    inverse = jnp.broadcast_to(1.0 / norm, (1, LANES))
    for chunk in range(std_ref.shape[0]):
        std_ref[chunk : chunk + 1, :] = back_ref[chunk + chunk // per] * inverse


def body(source_id, slot, owner, counts, partials, residual, weight, prior):
    axes = ("grp", "dev")
    peers = lax.axis_size("grp") * lax.axis_size("dev")
    params = partials.shape[0]
    row_count = residual.shape[0]
    src_local = counts.shape[0]
    pad_slots = row_count // src_local
    block_rows = row_count // peers
    chunks = row_count // LANES
    per = block_rows // LANES
    compact = per > 0 and per % QUAD == 0
    f32 = jnp.float32
    grid_of = lambda x: x.reshape(-1, LANES)
    send = lambda x: lax.all_to_all(x, axes, split_axis=0, concat_axis=0, tiled=True)
    vmem_spec = pl.BlockSpec(memory_space=pltpu.VMEM)
    wire_shape = (chunks // QUAD * (2 * QUAD - 1), QUAD, LANES) if compact else (chunks, SUB, LANES)
    wire = pl.pallas_call(
        lambda *refs: pack_kernel(*refs, src_local=src_local, pad_slots=pad_slots, compact=compact),
        out_shape=pltpu.VMEM(wire_shape, f32),
        name="pack_rows",
    )(grid_of(source_id), grid_of(slot), grid_of(owner), partials, grid_of(residual), grid_of(weight))
    if per:
        arrived = send(wire.reshape((peers, -1) + wire_shape[1:])).reshape(wire_shape)
    else:
        parts = LANES // block_rows
        cut = wire.reshape(chunks, SUB, parts, block_rows).transpose(0, 2, 1, 3)
        cut = send(cut.reshape(peers, SUB, block_rows))
        cut = cut.reshape(chunks, parts, SUB, block_rows).transpose(0, 2, 1, 3)
        arrived = cut.reshape(wire_shape)
    arrived = pltpu.with_memory_space_constraint(arrived, pltpu.VMEM)
    back_lines = peers * (per + 1) if per else chunks + 1
    updates, back = pl.pallas_call(
        lambda *refs: owner_kernel(*refs, pad_slots=pad_slots, per=per, compact=compact),
        out_shape=(
            jax.ShapeDtypeStruct((params, src_local), f32),
            pltpu.VMEM((back_lines, 1, LANES), f32),
        ),
        in_specs=[vmem_spec] * 3,
        scratch_shapes=[
            pltpu.VMEM((9 * SUB, src_local), f32),
            pltpu.VMEM((chunks, SUB, LANES), f32),
            pltpu.VMEM((chunks, SUB, LANES), jnp.int32),
        ],
        name="owner_fit",
    )(arrived, counts.reshape(1, -1), prior)
    if per:
        back = send(back.reshape(peers, per + 1, 1, LANES)).reshape(back_lines, 1, LANES)
        back = pltpu.with_memory_space_constraint(back, pltpu.VMEM)
        standardized, norm = pl.pallas_call(
            lambda *refs: finish_kernel(*refs, per=per),
            out_shape=(
                jax.ShapeDtypeStruct((chunks, LANES), f32),
                jax.ShapeDtypeStruct((1, 1), f32),
            ),
            in_specs=[vmem_spec],
            name="finish",
        )(back)
        return (updates, standardized.reshape(row_count), norm.reshape(()))
    back = back[:, 0, :]
    line = jnp.broadcast_to(back[chunks, 0:2][None], (peers, 2))
    back = send(jnp.concatenate([back[:chunks].reshape(peers, block_rows), line], axis=1))
    totals = jnp.sum(back[:, block_rows:], axis=0)
    norm = jnp.sqrt(totals[0] / totals[1] + 1e-06)
    return (updates, back[:, :block_rows].reshape(row_count) / norm, norm)


def solution(mesh):
    in_specs = (
        P(("grp", "dev")),
        P(("grp", "dev")),
        P(),
        P(("grp", "dev")),
        P(None, ("grp", "dev")),
        P(("grp", "dev")),
        P(("grp", "dev")),
        P(None, ("grp", "dev")),
    )
    out_specs = (P(None, ("grp", "dev")), P(("grp", "dev")), P())
    return jax.shard_map(body, mesh=mesh, in_specs=in_specs, out_specs=out_specs, check_vma=False)
```

```python
import jax
import jax.numpy as jnp
from jax import lax
from jax.experimental import pallas as pl
from jax.experimental.pallas import tpu as pltpu
from jax.sharding import PartitionSpec as P

LANES = 128
SUB = 8
QUAD = 4
STEP = 128
PART = 32


def pick_lanes(table, idx):
    return jnp.take_along_axis(table, idx, axis=1, mode="promise_in_bounds")


def split_index(value, size):
    if size & (size - 1) == 0:
        return lax.shift_right_logical(value, size.bit_length() - 1), value & (size - 1)
    return lax.div(value, size), lax.rem(value, size)


def pack_kernel(sid_ref, slot_ref, owner_ref, partials_ref, res_ref, wgt_ref, wire_ref, *, src_local, pad_slots, compact):
    params = partials_ref.shape[0]
    bits = max(1, (src_local - 1).bit_length())
    fit = 31 // bits
    tiles = owner_ref.shape[0] // SUB
    row_of = lax.broadcasted_iota(jnp.int32, (SUB, LANES), 0)

    def merged(first, count):
        line = jnp.zeros((SUB, LANES), jnp.int32)
        for t in range(count):
            here = owner_ref[pl.ds(pl.multiple_of((first + t) * SUB, SUB), SUB), :]
            line = line | (split_index(here, src_local)[1] << (t * bits))
        return line

    def look(first, count, high, low, pos):
        packed = merged(first, count)
        tile_id, line_id = split_index(high, SUB)
        found = jnp.zeros((SUB, LANES), jnp.int32)
        for s in range(SUB):
            line = jnp.broadcast_to(packed[s : s + 1, :], (SUB, LANES))
            found = jnp.where(line_id == s, pick_lanes(line, low), found)
        turn = tile_id - first
        inside = (turn >= 0) & (turn < count)
        moved = lax.shift_right_logical(found, jnp.where(inside, turn, 0) * bits) & ((1 << bits) - 1)
        return jnp.where(inside, moved, pos)

    def group(g, carry):
        base = pl.multiple_of(g * SUB, SUB)
        high, low = split_index(sid_ref[pl.ds(base, SUB), :], LANES)
        pos = jnp.zeros((SUB, LANES), jnp.int32)
        whole = tiles // fit
        if whole <= 1:
            for t in range(whole):
                pos = look(t * fit, fit, high, low, pos)
        else:
            pos = lax.fori_loop(0, whole, lambda t, p: look(t * fit, fit, high, low, p), pos)
        if tiles % fit:
            pos = look(whole * fit, tiles % fit, high, low, pos)
        cell = (pos * pad_slots + slot_ref[pl.ds(base, SUB), :]).astype(jnp.float32)
        root = jnp.sqrt(wgt_ref[pl.ds(base, SUB), :])
        res = res_ref[pl.ds(base, SUB), :] * root
        built = []
        for s in range(SUB):
            lane0 = pl.multiple_of((base + s) * LANES, LANES)
            slopes = partials_ref[:, pl.ds(lane0, LANES)] * root[s : s + 1, :]
            tile = jnp.concatenate([slopes, jnp.zeros((SUB - params, LANES), jnp.float32)], axis=0)
            tile = jnp.where(row_of == params, res[s : s + 1, :], tile)
            built.append(jnp.where(row_of == params + 1, cell[s : s + 1, :], tile))
        if not compact:
            for s in range(SUB):
                wire_ref[base + s] = built[s]
            return carry
        for quad in range(SUB // QUAD):
            last = built[quad * QUAD + QUAD - 1]
            line0 = (g * (SUB // QUAD) + quad) * (2 * QUAD - 1)
            for c in range(QUAD - 1):
                tile = jnp.where(row_of == SUB - 1, last[QUAD + c : QUAD + c + 1, :], built[quad * QUAD + c])
                wire_ref[line0 + 2 * c] = tile[0:QUAD]
                wire_ref[line0 + 2 * c + 1] = tile[QUAD:]
            wire_ref[line0 + 2 * QUAD - 2] = last[0:QUAD]
        return carry

    lax.fori_loop(0, sid_ref.shape[0] // SUB, group, 0, unroll=16)


def solve_rows(normal, moments):
    params = len(moments)
    raw, factor, inverse = {}, {}, []
    for column in range(params):
        for target in range(column, params):
            current = normal[target][column]
            for earlier in range(column):
                current = current - factor[target, earlier] * raw[column, earlier]
            raw[target, column] = current
        inverse.append(1.0 / raw[column, column])
        for target in range(column + 1, params):
            factor[target, column] = raw[target, column] * inverse[column]
    forward = []
    for target in range(params):
        current = moments[target]
        for earlier in range(target):
            current = current - factor[target, earlier] * forward[earlier]
        forward.append(current)
    backward = [None] * params
    for target in reversed(range(params)):
        current = forward[target] * inverse[target]
        for later in range(target + 1, params):
            current = current - factor[later, target] * backward[later]
        backward[target] = current
    return backward


def owner_kernel(wire_ref, counts_ref, prior_ref, upd_ref, out_ref, acc_ref, rows_ref, src_ref, *, pad_slots, per, compact):
    params = prior_ref.shape[0]
    chunks = rows_ref.shape[0]
    src_local = counts_ref.shape[1]
    row_of = lax.broadcasted_iota(jnp.int32, (SUB, LANES), 0)
    source_of = lax.broadcasted_iota(jnp.int32, (src_local, LANES), 0)
    counts = counts_ref[...]
    count_table = jnp.broadcast_to(counts, (SUB, src_local))
    acc_ref[...] = jnp.zeros_like(acc_ref)
    step = min(STEP, chunks)

    def tiles_of(index):
        if not compact:
            return [wire_ref[index * step + s] for s in range(step)]
        out = []
        for quad in range(step // QUAD):
            line0 = (index * (step // QUAD) + quad) * (2 * QUAD - 1)
            three = [
                jnp.concatenate([wire_ref[line0 + 2 * c], wire_ref[line0 + 2 * c + 1]], axis=0)
                for c in range(QUAD - 1)
            ]
            spare = [tile[SUB - 1 :, :] for tile in three]
            last = jnp.concatenate([wire_ref[line0 + 2 * QUAD - 2]] + spare + [spare[0]], axis=0)
            out += three + [last]
        return out

    def gather_sums(index, carry):
        lefts, hots = [], []
        for s, tile in enumerate(tiles_of(index)):
            chunk = index * step + s
            cell = jnp.broadcast_to(tile[params + 1 : params + 2, :].astype(jnp.int32), (SUB, LANES))
            source, slot = split_index(cell, pad_slots)
            rows = jnp.where(slot < pick_lanes(count_table, source), tile, 0.0)
            rows_ref[chunk] = rows
            src_ref[chunk] = source
            left = jnp.where(row_of < params, rows, rows[params : params + 1, :])
            turn = lambda shift: pltpu.roll(rows, shift, 0)
            right0 = jnp.where(row_of < params, rows, turn(5))
            right1 = jnp.where(row_of < 4, turn(7), jnp.where(row_of == 4, turn(4), turn(2)))
            right2 = jnp.where(row_of < 3, turn(6), turn(3))
            parts = [left * right0, left * right1, left * right2]
            pieces = []
            for _ in range(2):
                heads = [p.astype(jnp.bfloat16).astype(jnp.float32) for p in parts]
                pieces += heads
                parts = [p - h for p, h in zip(parts, heads)]
            lefts.append(jnp.concatenate(pieces + parts, axis=0).astype(jnp.bfloat16))
            hots.append((source_of == source[0:1, :]).astype(jnp.float32).astype(jnp.bfloat16))
        for first in range(0, step, PART):
            acc_ref[...] += lax.dot_general(
                jnp.concatenate(lefts[first : first + PART], axis=1),
                jnp.concatenate(hots[first : first + PART], axis=1),
                (((1,), (1,)), ((), ())),
                preferred_element_type=jnp.float32,
            )
        return carry

    lax.fori_loop(0, chunks // step, gather_sums, 0)
    width = 3 * SUB
    sums = acc_ref[0:width, :] + (acc_ref[width : 2 * width, :] + acc_ref[2 * width : 3 * width, :])
    line_at = lambda turn, row: sums[turn * SUB + row : turn * SUB + row + 1, :]
    normal = [[None] * params for _ in range(params)]
    for turn in range(3):
        for first_idx in range(params):
            second_idx = (first_idx + turn) % params
            entry = line_at(turn, first_idx)
            if turn == 0:
                entry = entry + prior_ref[first_idx : first_idx + 1, :]
            normal[first_idx][second_idx] = entry
            normal[second_idx][first_idx] = entry
    moments = [line_at(0, 5), line_at(0, 6), line_at(0, 7), line_at(1, 5), line_at(1, 6)]
    solved = solve_rows(normal, moments)
    table = jnp.where(row_of == params, 1.0, 0.0)
    for i in range(params):
        upd_ref[i : i + 1, :] = solved[i]
        table = jnp.where(row_of == i, -solved[i], table)

    def refit(index, total):
        for s in range(step):
            chunk = index * step + s
            fresh = jnp.sum(rows_ref[chunk] * pick_lanes(table, src_ref[chunk]), axis=0, keepdims=True)
            total = total + fresh * fresh
            out_ref[chunk + (chunk // per if per else 0)] = fresh
        return total

    total = lax.fori_loop(0, chunks // step, refit, jnp.zeros((1, LANES), jnp.float32))
    squares = jnp.sum(total, axis=1, keepdims=True)
    seen = jnp.sum(counts.astype(jnp.float32), axis=1, keepdims=True)
    lane_of = lax.broadcasted_iota(jnp.int32, (1, LANES), 1)
    line = jnp.where(lane_of == 0, squares, jnp.where(lane_of == 1, seen, 0.0))
    stride = per + 1 if per else chunks + 1
    for last in range(stride - 1, out_ref.shape[0], stride):
        out_ref[last] = line


def finish_kernel(back_ref, std_ref, norm_ref, *, per):
    stride = per + 1
    lines = [back_ref[last] for last in range(per, back_ref.shape[0], stride)]
    while len(lines) > 1:
        lines = [a + b for a, b in zip(lines[::2], lines[1::2])] + lines[len(lines) & ~1 :]
    lane_of = lax.broadcasted_iota(jnp.int32, (1, LANES), 1)
    squares = jnp.sum(jnp.where(lane_of == 0, lines[0], 0.0), axis=1, keepdims=True)
    seen = jnp.sum(jnp.where(lane_of == 1, lines[0], 0.0), axis=1, keepdims=True)
    norm = jnp.sqrt(squares / seen + 1e-06)
    norm_ref[...] = norm
    inverse = jnp.broadcast_to(1.0 / norm, (1, LANES))
    for chunk in range(std_ref.shape[0]):
        std_ref[chunk : chunk + 1, :] = back_ref[chunk + chunk // per] * inverse


def body(source_id, slot, owner, counts, partials, residual, weight, prior):
    axes = ("grp", "dev")
    peers = lax.axis_size("grp") * lax.axis_size("dev")
    params = partials.shape[0]
    row_count = residual.shape[0]
    src_local = counts.shape[0]
    pad_slots = row_count // src_local
    block_rows = row_count // peers
    chunks = row_count // LANES
    per = block_rows // LANES
    compact = per > 0 and per % QUAD == 0
    f32 = jnp.float32
    grid_of = lambda x: x.reshape(-1, LANES)
    send = lambda x: lax.all_to_all(x, axes, split_axis=0, concat_axis=0, tiled=True)
    vmem_spec = pl.BlockSpec(memory_space=pltpu.VMEM)
    wire_shape = (chunks // QUAD * (2 * QUAD - 1), QUAD, LANES) if compact else (chunks, SUB, LANES)
    wire = pl.pallas_call(
        lambda *refs: pack_kernel(*refs, src_local=src_local, pad_slots=pad_slots, compact=compact),
        out_shape=pltpu.VMEM(wire_shape, f32),
        name="pack_rows",
    )(grid_of(source_id), grid_of(slot), grid_of(owner), partials, grid_of(residual), grid_of(weight))
    if per:
        arrived = send(wire.reshape((peers, -1) + wire_shape[1:])).reshape(wire_shape)
    else:
        parts = LANES // block_rows
        cut = wire.reshape(chunks, SUB, parts, block_rows).transpose(0, 2, 1, 3)
        cut = send(cut.reshape(peers, SUB, block_rows))
        cut = cut.reshape(chunks, parts, SUB, block_rows).transpose(0, 2, 1, 3)
        arrived = cut.reshape(wire_shape)
    arrived = pltpu.with_memory_space_constraint(arrived, pltpu.VMEM)
    back_lines = peers * (per + 1) if per else chunks + 1
    updates, back = pl.pallas_call(
        lambda *refs: owner_kernel(*refs, pad_slots=pad_slots, per=per, compact=compact),
        out_shape=(
            jax.ShapeDtypeStruct((params, src_local), f32),
            pltpu.VMEM((back_lines, 1, LANES), f32),
        ),
        in_specs=[vmem_spec] * 3,
        scratch_shapes=[
            pltpu.VMEM((9 * SUB, src_local), f32),
            pltpu.VMEM((chunks, SUB, LANES), f32),
            pltpu.VMEM((chunks, SUB, LANES), jnp.int32),
        ],
        name="owner_fit",
    )(arrived, counts.reshape(1, -1), prior)
    if per:
        back = send(back.reshape(peers, per + 1, 1, LANES)).reshape(back_lines, 1, LANES)
        back = pltpu.with_memory_space_constraint(back, pltpu.VMEM)
        standardized, norm = pl.pallas_call(
            lambda *refs: finish_kernel(*refs, per=per),
            out_shape=(
                jax.ShapeDtypeStruct((chunks, LANES), f32),
                jax.ShapeDtypeStruct((1, 1), f32),
            ),
            in_specs=[vmem_spec],
            name="finish",
        )(back)
        return (updates, standardized.reshape(row_count), norm.reshape(()))
    back = back[:, 0, :]
    line = jnp.broadcast_to(back[chunks, 0:2][None], (peers, 2))
    back = send(jnp.concatenate([back[:chunks].reshape(peers, block_rows), line], axis=1))
    totals = jnp.sum(back[:, block_rows:], axis=0)
    norm = jnp.sqrt(totals[0] / totals[1] + 1e-06)
    return (updates, back[:, :block_rows].reshape(row_count) / norm, norm)


def solution(mesh):
    in_specs = (
        P(("grp", "dev")),
        P(("grp", "dev")),
        P(),
        P(("grp", "dev")),
        P(None, ("grp", "dev")),
        P(("grp", "dev")),
        P(("grp", "dev")),
        P(None, ("grp", "dev")),
    )
    out_specs = (P(None, ("grp", "dev")), P(("grp", "dev")), P())
    return jax.shard_map(body, mesh=mesh, in_specs=in_specs, out_specs=out_specs, check_vma=False)
```
